8 devices in a mesh: nodes: 8 (over z, y, x, core).
Axes of the slice: x: 2, y: 2, z: 1, core: 2. Of those that a mesh axis runs over, the one named last changes fastest.
Arguments:
- adjacency: bfloat16 [16384, 16384], P('nodes')
- features: bfloat16 [16384, 602], P('nodes')
- w_one: float32 [602, 128], replicated
- w_two: float32 [128, 41], replicated
- labels: int32 [16384], P('nodes')
- label_mask: int32 [16384], P('nodes')
Outputs:
- output 1: float32 [], replicated
- output 2: float32 [602, 128], replicated
- output 3: float32 [128, 41], replicated
All inputs are finite; a program needn't handle non-finite values.
Results may differ from the reference program's by a relative error of at most 0.0021.
Values are sent between devices in bfloat16 or wider.
A program may use at most 1 GiB of HBM per device.

```python
import jax
import jax.numpy as jnp
from jax import lax

NUM_NODES = 16384
F_IN = 602
HIDDEN = 128
CLASSES = 41
COMMUNITIES = 8
EDGE_IN = 40
EDGE_OUT = 8
HASH_MOD = 128
HASH_SHIFT = 2048
HASH_RANGE = 32768
LABEL_RATE = 4


def draw_graph(key_base):
    key_mult, key_add, key_comm = jax.random.split(key_base, 3)
    mult_ids = jax.random.randint(key_mult, (NUM_NODES,), 0, HASH_RANGE, dtype=jnp.int32)
    add_ids = jax.random.randint(key_add, (NUM_NODES,), 0, HASH_RANGE, dtype=jnp.int32)
    comm_ids = jax.random.randint(key_comm, (NUM_NODES,), 0, COMMUNITIES, dtype=jnp.int32)
    hashed = (mult_ids[:, None] * mult_ids[None, :] // HASH_SHIFT + add_ids[:, None] + add_ids[None, :]) % HASH_MOD
    edge_limit = jnp.where(comm_ids[:, None] == comm_ids[None, :], EDGE_IN, EDGE_OUT)
    node_ids = jnp.arange(NUM_NODES, dtype=jnp.int32)
    linked = (hashed < edge_limit) | (node_ids[:, None] == node_ids[None, :])
    degree = jnp.sum(linked.astype(jnp.int32), axis=1).astype(jnp.float32)
    inv_root = lax.rsqrt(degree)
    adjacency = jnp.where(linked, inv_root[:, None] * inv_root[None, :], 0.0).astype(jnp.bfloat16)
    return adjacency, jnp.sqrt(jnp.mean(degree))


def draw_mask(key_base):
    key_rate, key_pick = jax.random.split(key_base)
    chosen = jax.random.randint(key_rate, (NUM_NODES,), 0, LABEL_RATE, dtype=jnp.int32) == 0
    forced = jax.random.randint(key_pick, (), 0, NUM_NODES, dtype=jnp.int32)
    return (chosen | (jnp.arange(NUM_NODES, dtype=jnp.int32) == forced)).astype(jnp.int32)


def setup_inputs(seed: int = 0) -> dict:
    key_base = jax.random.key(seed)
    key_graph, key_feat, key_one, key_two, key_label, key_mask = jax.random.split(key_base, 6)
    adjacency, weight_gain = draw_graph(key_graph)
    features = jax.random.normal(key_feat, (NUM_NODES, F_IN), jnp.float32).astype(jnp.bfloat16)
    w_one = jax.random.normal(key_one, (F_IN, HIDDEN), jnp.float32) * (weight_gain * F_IN ** -0.5)
    raw_two = jax.random.normal(key_two, (HIDDEN, CLASSES), jnp.float32)
    w_two = (raw_two - jnp.mean(raw_two, axis=0, keepdims=True)) * (1.5 * weight_gain * HIDDEN ** -0.5)
    labels = jax.random.randint(key_label, (NUM_NODES,), 0, CLASSES, dtype=jnp.int32)
    label_mask = draw_mask(key_mask)
    return {'adjacency': adjacency, 'features': features, 'w_one': w_one, 'w_two': w_two, 'labels': labels, 'label_mask': label_mask}


def contract_rows(left, right):
    return lax.dot_general(left, right, (((0,), (0,)), ((), ())), preferred_element_type=jnp.float32)


def reference(adjacency, features, w_one, w_two, labels, label_mask):
    w_one_b = w_one.astype(jnp.bfloat16)
    w_two_b = w_two.astype(jnp.bfloat16)
    y_one = jnp.dot(features, w_one_b, preferred_element_type=jnp.float32).astype(jnp.bfloat16)
    z_one = jnp.dot(adjacency, y_one, preferred_element_type=jnp.float32)
    h_one = jnp.maximum(z_one, 0.0).astype(jnp.bfloat16)
    y_two = jnp.dot(h_one, w_two_b, preferred_element_type=jnp.float32).astype(jnp.bfloat16)
    z_two = jnp.dot(adjacency, y_two, preferred_element_type=jnp.float32)
    mask_f = label_mask.astype(jnp.float32)
    label_count = jnp.sum(mask_f)
    log_norm = jax.nn.logsumexp(z_two, axis=1)
    onehot = (labels[:, None] == jnp.arange(CLASSES, dtype=jnp.int32)[None, :]).astype(jnp.float32)
    picked = jnp.sum(z_two * onehot, axis=1)
    loss_value = jnp.sum(mask_f * (log_norm - picked)) / label_count
    soft_probs = jnp.exp(z_two - log_norm[:, None])
    g_two = ((soft_probs - onehot) * (mask_f / label_count)[:, None]).astype(jnp.bfloat16)
    grad_y2 = contract_rows(adjacency, g_two).astype(jnp.bfloat16)
    grad_two = contract_rows(h_one, grad_y2)
    grad_h1 = lax.dot_general(grad_y2, w_two_b, (((1,), (1,)), ((), ())), preferred_element_type=jnp.float32)
    grad_z1 = jnp.where(z_one > 0.0, grad_h1, 0.0).astype(jnp.bfloat16)
    grad_y1 = contract_rows(adjacency, grad_z1).astype(jnp.bfloat16)
    grad_one = contract_rows(features, grad_y1)
    return (loss_value, grad_one, grad_two)
```

```python
import jax
import jax.numpy as jnp
from jax import lax
from jax.sharding import PartitionSpec as P


def contract_rows(left, right):
    return lax.dot_general(left, right, (((0,), (0,)), ((), ())), preferred_element_type=jnp.float32)


def solution(mesh):
    node_axis = mesh.axis_names[0]

    def local_step(adj_rows, feat_rows, w_one, w_two, label_rows, mask_rows):
        classes = w_two.shape[1]
        w_one_b = w_one.astype(jnp.bfloat16)
        w_two_b = w_two.astype(jnp.bfloat16)
        y_one = jnp.dot(feat_rows, w_one_b, preferred_element_type=jnp.float32).astype(jnp.bfloat16)
        y_one_all = lax.all_gather(y_one, node_axis, tiled=True)
        z_one = jnp.dot(adj_rows, y_one_all, preferred_element_type=jnp.float32)
        h_one = jnp.maximum(z_one, 0.0).astype(jnp.bfloat16)
        y_two = jnp.dot(h_one, w_two_b, preferred_element_type=jnp.float32).astype(jnp.bfloat16)
        y_two_all = lax.all_gather(y_two, node_axis, tiled=True)
        z_two = jnp.dot(adj_rows, y_two_all, preferred_element_type=jnp.float32)
        mask_f = mask_rows.astype(jnp.float32)
        label_count = lax.psum(jnp.sum(mask_f), node_axis)
        log_norm = jax.nn.logsumexp(z_two, axis=1)
        onehot = (label_rows[:, None] == jnp.arange(classes, dtype=jnp.int32)[None, :]).astype(jnp.float32)
        picked = jnp.sum(z_two * onehot, axis=1)
        loss_value = lax.psum(jnp.sum(mask_f * (log_norm - picked)), node_axis) / label_count
        soft_probs = jnp.exp(z_two - log_norm[:, None])
        g_two = ((soft_probs - onehot) * (mask_f / label_count)[:, None]).astype(jnp.bfloat16)
        g_two_all = lax.all_gather(g_two, node_axis, tiled=True)
        grad_y2 = jnp.dot(adj_rows, g_two_all, preferred_element_type=jnp.float32).astype(jnp.bfloat16)
        grad_two = lax.psum(contract_rows(h_one, grad_y2), node_axis)
        grad_h1 = lax.dot_general(grad_y2, w_two_b, (((1,), (1,)), ((), ())), preferred_element_type=jnp.float32)
        grad_z1 = jnp.where(z_one > 0.0, grad_h1, 0.0).astype(jnp.bfloat16)
        grad_z1_all = lax.all_gather(grad_z1, node_axis, tiled=True)
        grad_y1 = jnp.dot(adj_rows, grad_z1_all, preferred_element_type=jnp.float32).astype(jnp.bfloat16)
        grad_one = lax.psum(contract_rows(feat_rows, grad_y1), node_axis)
        return loss_value, grad_one, grad_two

    return jax.shard_map(local_step, mesh=mesh, in_specs=(P(node_axis, None), P(node_axis, None), P(None, None), P(None, None), P(node_axis), P(node_axis)), out_specs=(P(), P(None, None), P(None, None)), check_vma=False)
```

```python
import functools

import jax
import jax.numpy as jnp
from jax import lax
from jax.experimental import pallas as pl
from jax.experimental.pallas import tpu as pltpu
from jax.sharding import PartitionSpec as P

BF = jnp.bfloat16
F32 = jnp.float32
MESH = pl.DeviceIdType.MESH
NB = 3
XS, YS, XO, YO, ZS, ZO = range(6)


def dot_nn(a, b):
    return lax.dot_general(a, b, (((1,), (0,)), ((), ())), preferred_element_type=F32)


def dot_nt(a, b):
    return lax.dot_general(a, b, (((1,), (1,)), ((), ())), preferred_element_type=F32)


def kernel(dims, adj, feat, w1_ref, w2_ref, lab_ref, msk_ref, out_ref,
           ring, res, wide, thin, accs, precv, precv_thin, xbuf, h1, cnt_s, cnt_r, w2p,
           fin, fr1, half, fr2, fin_all,
           ring_sem, res_sem, x_sem, g_send, g_recv, p_send, p_recv, c_send, c_recv, f_send, f_recv):
    rows, width, hidden, classes = dims
    cpad = thin.shape[3]
    nch = 4
    ck = rows // nch
    me = lax.axis_index("nodes")
    core = lax.rem(me, 2)
    chip = me // 2
    xc = chip + 1 - 2 * lax.rem(chip, 2)
    yc = lax.rem(chip + 2, 4)
    zc = 3 - chip
    other = 1 - core
    part = chip * 2 + other
    xs, xo, ys, yo, zs, zo = (xc * 2 + core, xc * 2 + other, yc * 2 + core, yc * 2 + other,
                              zc * 2 + core, zc * 2 + other)
    dev_of = (xs, ys, xo, yo, zs, zo)

    def ring_copy(t):
        m = lax.rem(t, 12)
        b, q = m // 4, lax.rem(m, 4)
        e = ((1 - b) * (2 - b) // 2) * me + b * (2 - b) * part + (b * (b - 1) // 2) * zo
        slot = lax.rem(t, NB)
        cols = pl.ds(pl.multiple_of(e * rows + q * ck, ck), ck)
        return pltpu.make_async_copy(adj.at[:, cols], ring.at[slot], ring_sem.at[slot])

    def res_copy(r, q):
        cols = pl.ds(pl.multiple_of(dev_of[r] * rows + q * ck, ck), ck)
        return pltpu.make_async_copy(adj.at[:, cols], res.at[r * 4 + q], res_sem.at[r * 4 + q])

    x_copy = pltpu.make_async_copy(feat, xbuf, x_sem)
    x_copy.start()
    for t in range(NB):
        ring_copy(t).start()
    for q in range(nch):
        for r in (XS, YS, XO, YO):
            res_copy(r, q).start()
    for q in range(nch):
        res_copy(ZS, q).start()

    barrier = pltpu.get_barrier_semaphore()
    for o in range(1, 8):
        pl.semaphore_signal(barrier, inc=1, device_id=(lax.rem(me + o, 8),), device_id_type=MESH)

    mask_f = msk_ref[...].astype(F32)
    cnt_s[...] = jnp.broadcast_to(jnp.sum(mask_f, axis=1, keepdims=True), (8, 128))
    w1t = w1_ref[...].astype(BF).T
    w2p[...] = jnp.zeros_like(w2p)
    w2p[:, pl.ds(0, classes)] = w2_ref[...]
    w2b = w2p[:, pl.ds(0, cpad)].astype(BF)
    w2t = w2p[...].T[:cpad].astype(BF)
    pl.semaphore_wait(barrier, 7)

    def cnt_copy(o):
        return pltpu.make_async_remote_copy(cnt_s, cnt_r.at[o], c_send.at[o], c_recv.at[o],
                                            device_id=(lax.rem(me + o, 8),), device_id_type=MESH)

    def rdma(src, dst, ss, rs, dev):
        return pltpu.make_async_remote_copy(src, dst, ss, rs, device_id=(dev,), device_id_type=MESH)

    def gather_send(pi, buf):
        for q in range(nch):
            rdma(buf.at[me, q], buf.at[me, q], g_send.at[pi, 0, q], g_recv.at[pi, XS, q], xs).start()
            rdma(buf.at[me, q], buf.at[me, q], g_send.at[pi, 1, q], g_recv.at[pi, YS, q], ys).start()

    def run_pass(pi, n, buf, prv):
        gather_send(pi, buf)
        if pi == 0:
            for o in range(1, 8):
                cnt_copy(o).start()

        def local(m, _):
            t = pi * 12 + m
            b, q = m // 4, lax.rem(m, 4)
            ring_copy(t).wait()
            slot = lax.rem(t, NB)
            total = dot_nn(buf[me, 0], ring[slot, pl.ds(0, ck)])
            for c in range(1, nch):
                total += dot_nn(buf[me, c], ring[slot, pl.ds(c * ck, ck)])
            accs[b, pl.ds(0, n), pl.ds(pl.multiple_of(q * ck, ck), ck)] = total

            ring_copy(t + NB).start()
            return 0

        lax.fori_loop(0, 8, local, 0)
        p_copy = rdma(accs.at[1, pl.ds(0, n)], prv, p_send.at[pi], p_recv.at[pi], part)
        p_copy.start()

        def recv(r, q):
            return rdma(buf.at[dev_of[r], q], buf.at[dev_of[r], q], g_send.at[pi, 0, q], g_recv.at[pi, r, q], me)

        def relay(r, q):
            to = {XS: XO, YS: YO, ZS: ZO}[r]
            return rdma(buf.at[dev_of[r], q], buf.at[dev_of[r], q], g_send.at[pi, {XS: 2, YS: 3, ZS: 4}[r], q],
                        g_recv.at[pi, to, q], part)

        def forward(q, src, to):
            return rdma(buf.at[src, q], buf.at[src, q], g_send.at[pi, 5, q], g_recv.at[pi, ZS, q], to)

        def add(*terms):
            for i in range(nch):
                here = pl.ds(i * ck, ck)
                s = accs[0, pl.ds(0, n), here]
                for v, a in terms:
                    s += dot_nt(v, a[here, :])
                accs[0, pl.ds(0, n), here] = s

        def loaded(r, q):
            if pi == 0:
                res_copy(r, q).wait()
            return buf[dev_of[r], q], res.at[r * 4 + q]

        def near(q, _):
            recv(XS, q).wait_recv()
            relay(XS, q).start()

            @pl.when(q < 2)
            def _():
                forward(q, xs, ys).start()
            recv(YS, q).wait_recv()
            relay(YS, q).start()

            @pl.when(q >= 2)
            def _():
                forward(q, ys, xs).start()
            add(loaded(XS, q), loaded(YS, q))
            recv(XO, q).wait_recv()
            recv(YO, q).wait_recv()
            add(loaded(XO, q), loaded(YO, q))
            return 0

        lax.fori_loop(0, nch, near, 0)

        def far(q, _):
            recv(ZS, q).wait_recv()
            relay(ZS, q).start()
            add(loaded(ZS, q))
            t = pi * 12 + 8 + q
            ring_copy(t).wait()
            recv(ZO, q).wait_recv()
            add((buf[zo, q], ring.at[lax.rem(t, NB)]))

            if pi < 3:
                ring_copy(t + NB).start()
            else:
                @pl.when(q < nch - NB)
                def _():
                    ring_copy(t + NB).start()
            return 0

        lax.fori_loop(0, nch, far, 0)

        def drain(q, _):
            for i in range(6):
                rdma(buf.at[me, q], buf.at[me, q], g_send.at[pi, i, q], g_recv.at[pi, 0, q], me).wait_send()
            return 0

        lax.fori_loop(0, nch, drain, 0)
        p_copy.wait()

    x_copy.wait()
    for q in range(nch):
        wide[me, q] = dot_nt(w1t, xbuf[pl.ds(q * ck, ck)]).astype(BF)
    run_pass(0, hidden, wide, precv)

    for q in range(nch):
        here = pl.ds(q * ck, ck)
        h = jnp.maximum(accs[0, :, here] + precv[:, here], 0.0).astype(BF)
        h1[:, here] = h
        thin[0, me, q] = dot_nn(w2t, h).astype(BF)
    run_pass(1, cpad, thin.at[0], precv_thin.at[0])

    count = cnt_s[...]
    for o in range(1, 8):
        cnt_copy(o).wait()
        count += cnt_r[o]
    count = count[0:1, 0:1]
    loss_part = jnp.zeros((1, 1), F32)
    cls = lax.broadcasted_iota(jnp.int32, (cpad, ck), 0)
    real = cls < classes
    for q in range(nch):
        here = pl.ds(q * ck, ck)
        z2 = accs[0, pl.ds(0, cpad), here] + precv_thin[0, :, here]
        top = jnp.max(jnp.where(real, z2, -jnp.inf), axis=0, keepdims=True)
        total = jnp.sum(jnp.where(real, jnp.exp(z2 - top), 0.0), axis=0, keepdims=True)
        log_norm = top + jnp.log(total)
        hot = cls == lab_ref[:, here]
        picked = jnp.sum(jnp.where(hot, z2, 0.0), axis=0, keepdims=True)
        mask_f = msk_ref[:, here].astype(F32)
        loss_part += jnp.sum(mask_f * (log_norm - picked), axis=1, keepdims=True)
        soft = jnp.exp(z2 - log_norm)
        g2 = (soft - hot.astype(F32)) * (mask_f / count)
        thin[1, me, q] = jnp.where(real, g2, 0.0).astype(BF)
    run_pass(2, cpad, thin.at[1], precv_thin.at[1])

    d2 = jnp.zeros((hidden, cpad), F32)
    for q in range(nch):
        here = pl.ds(q * ck, ck)
        e2 = (accs[0, pl.ds(0, cpad), here] + precv_thin[1, :, here]).astype(BF)
        d2 += dot_nt(h1[:, here], e2)
        gh = dot_nn(w2b, e2)
        wide[me, q] = jnp.where(h1[:, here] > 0, gh, 0.0).astype(BF)
    col = lax.broadcasted_iota(jnp.int32, (hidden, cpad), 1)
    d2 = jnp.where(col == classes, loss_part / count, d2)
    run_pass(3, hidden, wide, precv)

    for q in range(nch):
        here = pl.ds(q * ck, ck)
        h1[:, here] = (accs[0, :, here] + precv[:, here]).astype(BF)
    fin[:, pl.ds(0, width)] = dot_nn(h1[...], xbuf[...])
    fin[:, pl.ds(width, fin.shape[1] - width)] = jnp.zeros((hidden, fin.shape[1] - width), F32)
    fin[:, pl.ds(fin.shape[1] - 128, cpad)] = d2

    hh, qq = hidden // 2, hidden // 8
    c0 = rdma(fin.at[pl.ds(pl.multiple_of(other * hh, hh), hh)], fr1, f_send.at[0], f_recv.at[0], part)
    c0.start()
    c0.wait()
    half[...] = fin[pl.ds(pl.multiple_of(core * hh, hh), hh)] + fr1[...]
    copies = []
    for i, (c, dev) in enumerate(((zc, zs), (xc, xs), (yc, ys))):
        cp = rdma(half.at[pl.ds(pl.multiple_of(c * qq, qq), qq)], fr2.at[i], f_send.at[1 + i], f_recv.at[1 + i], dev)
        cp.start()
        copies.append(cp)
    for cp in copies:
        cp.wait()
    mine = half[pl.ds(pl.multiple_of(chip * qq, qq), qq)] + (fr2[0] + fr2[1] + fr2[2])
    fin_all[me] = mine
    copies = []
    for i, dev in enumerate((zs, xs, ys, part)):
        cp = rdma(fin_all.at[me], fin_all.at[me], f_send.at[4 + i], f_recv.at[4 + i], dev)
        cp.start()
        copies.append(cp)
    back = []
    for i, dev in ((1, xs), (2, ys), (0, zs)):
        rdma(fin_all.at[dev], fin_all.at[dev], f_send.at[4 + i], f_recv.at[4 + i], me).wait_recv()
        cp = rdma(fin_all.at[dev], fin_all.at[dev], f_send.at[8 + i], f_recv.at[8 + i], part)
        cp.start()
        back.append(cp)
    rdma(fin_all.at[part], fin_all.at[part], f_send.at[7], f_recv.at[7], me).wait_recv()
    for i, dev in ((1, xo), (2, yo), (0, zo)):
        rdma(fin_all.at[dev], fin_all.at[dev], f_send.at[8 + i], f_recv.at[8 + i], me).wait_recv()
    for cp in copies + back:
        cp.wait_send()
    for d in range(8):
        out_ref[pl.ds((d % 2) * hh + (d // 2) * qq, qq)] = fin_all[d]


def solution(mesh):
    def local_step(adj_rows, feat_rows, w_one, w_two, label_rows, mask_rows):
        rows, nodes = adj_rows.shape
        width, hidden = w_one.shape
        classes = w_two.shape[1]
        cpad = (classes + 1 + 15) // 16 * 16
        ck = rows // 4
        fw = (width + 127) // 128 * 128 + 128
        dims = (rows, width, hidden, classes)
        vm = pl.BlockSpec(memory_space=pltpu.VMEM)
        hb = pl.BlockSpec(memory_space=pl.ANY)
        dma = pltpu.SemaphoreType.DMA
        with jax.named_scope("gcn"):
            out = pl.pallas_call(
                functools.partial(kernel, dims),
                out_shape=jax.ShapeDtypeStruct((hidden, fw), F32),
                in_specs=[hb, hb, vm, vm, vm, vm],
                out_specs=vm,
                scratch_shapes=[
                    pltpu.VMEM((NB, rows, ck), BF),
                    pltpu.VMEM((20, rows, ck), BF),
                    pltpu.VMEM((8, 4, hidden, ck), BF),
                    pltpu.VMEM((2, 8, 4, cpad, ck), BF),
                    pltpu.VMEM((2, hidden, rows), F32),
                    pltpu.VMEM((hidden, rows), F32),
                    pltpu.VMEM((2, cpad, rows), F32),
                    pltpu.VMEM((rows, width), BF),
                    pltpu.VMEM((hidden, rows), BF),
                    pltpu.VMEM((8, 128), F32),
                    pltpu.VMEM((8, 8, 128), F32),
                    pltpu.VMEM((hidden, 128), F32),
                    pltpu.VMEM((hidden, fw), F32),
                    pltpu.VMEM((hidden // 2, fw), F32),
                    pltpu.VMEM((hidden // 2, fw), F32),
                    pltpu.VMEM((3, hidden // 8, fw), F32),
                    pltpu.VMEM((8, hidden // 8, fw), F32),
                    dma((NB,)), dma((20,)), dma,
                    dma((4, 6, 4)), dma((4, 6, 4)), dma((4,)), dma((4,)), dma((8,)), dma((8,)), dma((11,)), dma((11,)),
                ],
                compiler_params=pltpu.CompilerParams(
                    collective_id=0, has_side_effects=True, vmem_limit_bytes=67043328
                ),
            )(adj_rows, feat_rows, w_one, w_two, label_rows.reshape(1, rows), mask_rows.reshape(1, rows))
        grad_one = out[:, :width].T
        return out[0, fw - 128 + classes], grad_one, out[:, fw - 128:fw - 128 + classes]

    ax = mesh.axis_names[0]
    return jax.shard_map(local_step, mesh=mesh, in_specs=(P(ax, None), P(ax, None), P(None, None), P(None, None), P(ax), P(ax)),
                         out_specs=(P(), P(None, None), P(None, None)), check_vma=False)
```

```python
import functools

import jax
import jax.numpy as jnp
from jax import lax
from jax.experimental import pallas as pl
from jax.experimental.pallas import tpu as pltpu
from jax.sharding import PartitionSpec as P

BF = jnp.bfloat16
F32 = jnp.float32
MESH = pl.DeviceIdType.MESH
NB = 3
XS, YS, XO, YO, ZS, ZO = range(6)


def dot_nn(a, b):
    return lax.dot_general(a, b, (((1,), (0,)), ((), ())), preferred_element_type=F32)


def dot_nt(a, b):
    return lax.dot_general(a, b, (((1,), (1,)), ((), ())), preferred_element_type=F32)


def kernel(dims, adj, feat, w1_ref, w2_ref, lab_ref, msk_ref, out_ref,
           ring, res, wide, thin, accs, precv, precv_thin, xbuf, h1, cnt_s, cnt_r, w2p,
           fin, fr1, half, fr2, fin_all,
           ring_sem, res_sem, x_sem, g_send, g_recv, p_send, p_recv, c_send, c_recv, f_send, f_recv):
    rows, width, hidden, classes = dims
    cpad = thin.shape[3]
    w8 = (width + 7) // 8 * 8
    nch = 4
    ck = rows // nch
    me = lax.axis_index("nodes")
    core = lax.rem(me, 2)
    chip = me // 2
    xc = chip + 1 - 2 * lax.rem(chip, 2)
    yc = lax.rem(chip + 2, 4)
    zc = 3 - chip
    other = 1 - core
    part = chip * 2 + other
    xs, xo, ys, yo, zs, zo = (xc * 2 + core, xc * 2 + other, yc * 2 + core, yc * 2 + other,
                              zc * 2 + core, zc * 2 + other)
    dev_of = (xs, ys, xo, yo, zs, zo)

    def ring_copy(t):
        m = lax.rem(t, 12)
        b, q = m // 4, lax.rem(m, 4)
        e = ((1 - b) * (2 - b) // 2) * me + b * (2 - b) * part + (b * (b - 1) // 2) * zo
        slot = lax.rem(t, NB)
        cols = pl.ds(pl.multiple_of(e * rows + q * ck, ck), ck)
        return pltpu.make_async_copy(adj.at[:, cols], ring.at[slot], ring_sem.at[slot])

    def res_copy(r, q):
        cols = pl.ds(pl.multiple_of(dev_of[r] * rows + q * ck, ck), ck)
        return pltpu.make_async_copy(adj.at[:, cols], res.at[r * 4 + q], res_sem.at[r * 4 + q])

    x_copy = pltpu.make_async_copy(feat, xbuf, x_sem)
    x_copy.start()
    for t in range(NB):
        ring_copy(t).start()
    for q in range(nch):
        for r in (XS, YS, XO, YO):
            res_copy(r, q).start()
    for q in range(nch):
        res_copy(ZS, q).start()

    barrier = pltpu.get_barrier_semaphore()
    for o in range(1, 8):
        pl.semaphore_signal(barrier, inc=1, device_id=(lax.rem(me + o, 8),), device_id_type=MESH)

    mask_f = msk_ref[...].astype(F32)
    cnt_s[...] = jnp.broadcast_to(jnp.sum(mask_f, axis=1, keepdims=True), (8, 128))
    w1t = w1_ref[...].astype(BF).T
    w2p[...] = jnp.zeros_like(w2p)
    w2p[pl.ds(0, classes)] = w2_ref[...]
    w2t = w2p[pl.ds(0, cpad)].astype(BF)
    w2b = w2p[...].T[:, :cpad].astype(BF)
    pl.semaphore_wait(barrier, 7)

    def cnt_copy(o):
        return pltpu.make_async_remote_copy(cnt_s, cnt_r.at[o], c_send.at[o], c_recv.at[o],
                                            device_id=(lax.rem(me + o, 8),), device_id_type=MESH)

    def rdma(src, dst, ss, rs, dev):
        return pltpu.make_async_remote_copy(src, dst, ss, rs, device_id=(dev,), device_id_type=MESH)

    def gather_send(pi, buf):
        for q in range(nch):
            rdma(buf.at[me, q], buf.at[me, q], g_send.at[pi, 0, q], g_recv.at[pi, XS, q], xs).start()
            rdma(buf.at[me, q], buf.at[me, q], g_send.at[pi, 1, q], g_recv.at[pi, YS, q], ys).start()

    def run_pass(pi, n, buf, prv):
        gather_send(pi, buf)
        if pi == 0:
            for o in range(1, 8):
                cnt_copy(o).start()

        def local(m, _):
            t = pi * 12 + m
            b, q = m // 4, lax.rem(m, 4)
            ring_copy(t).wait()
            slot = lax.rem(t, NB)
            total = dot_nn(buf[me, 0], ring[slot, pl.ds(0, ck)])
            for c in range(1, nch):
                total += dot_nn(buf[me, c], ring[slot, pl.ds(c * ck, ck)])
            accs[b, pl.ds(0, n), pl.ds(pl.multiple_of(q * ck, ck), ck)] = total

            ring_copy(t + NB).start()
            return 0

        lax.fori_loop(0, 8, local, 0)
        p_copy = rdma(accs.at[1, pl.ds(0, n)], prv, p_send.at[pi], p_recv.at[pi], part)
        p_copy.start()

        def recv(r, q):
            return rdma(buf.at[dev_of[r], q], buf.at[dev_of[r], q], g_send.at[pi, 0, q], g_recv.at[pi, r, q], me)

        def relay(r, q):
            to = {XS: XO, YS: YO, ZS: ZO}[r]
            return rdma(buf.at[dev_of[r], q], buf.at[dev_of[r], q], g_send.at[pi, {XS: 2, YS: 3, ZS: 4}[r], q],
                        g_recv.at[pi, to, q], part)

        def forward(q, src, to):
            return rdma(buf.at[src, q], buf.at[src, q], g_send.at[pi, 5, q], g_recv.at[pi, ZS, q], to)

        def add(*terms):
            for i in range(nch):
                here = pl.ds(i * ck, ck)
                s = accs[0, pl.ds(0, n), here]
                for v, a in terms:
                    s += dot_nt(v, a[here, :])
                accs[0, pl.ds(0, n), here] = s

        def loaded(r, q):
            if pi == 0:
                res_copy(r, q).wait()
            return buf[dev_of[r], q], res.at[r * 4 + q]

        def near(q, _):
            recv(XS, q).wait_recv()
            relay(XS, q).start()

            @pl.when(q < 2)
            def _():
                forward(q, xs, ys).start()
            recv(YS, q).wait_recv()
            relay(YS, q).start()

            @pl.when(q >= 2)
            def _():
                forward(q, ys, xs).start()
            add(loaded(XS, q), loaded(YS, q))
            recv(XO, q).wait_recv()
            recv(YO, q).wait_recv()
            add(loaded(XO, q), loaded(YO, q))
            return 0

        lax.fori_loop(0, nch, near, 0)

        def far(q, _):
            recv(ZS, q).wait_recv()
            relay(ZS, q).start()
            add(loaded(ZS, q))
            t = pi * 12 + 8 + q
            ring_copy(t).wait()
            recv(ZO, q).wait_recv()
            add((buf[zo, q], ring.at[lax.rem(t, NB)]))

            if pi < 3:
                ring_copy(t + NB).start()
            else:
                @pl.when(q < nch - NB)
                def _():
                    ring_copy(t + NB).start()
            return 0

        lax.fori_loop(0, nch, far, 0)

        def drain(q, _):
            for i in range(6):
                rdma(buf.at[me, q], buf.at[me, q], g_send.at[pi, i, q], g_recv.at[pi, 0, q], me).wait_send()
            return 0

        lax.fori_loop(0, nch, drain, 0)
        p_copy.wait()

    x_copy.wait()
    for q in range(nch):
        wide[me, q] = dot_nn(w1t, xbuf[:, pl.ds(q * ck, ck)]).astype(BF)
    run_pass(0, hidden, wide, precv)

    for q in range(nch):
        here = pl.ds(q * ck, ck)
        h = jnp.maximum(accs[0, :, here] + precv[:, here], 0.0).astype(BF)
        h1[:, here] = h
        thin[0, me, q] = dot_nn(w2t, h).astype(BF)
    run_pass(1, cpad, thin.at[0], precv_thin.at[0])

    count = cnt_s[...]
    for o in range(1, 8):
        cnt_copy(o).wait()
        count += cnt_r[o]
    count = count[0:1, 0:1]
    loss_part = jnp.zeros((1, 1), F32)
    cls = lax.broadcasted_iota(jnp.int32, (cpad, ck), 0)
    real = cls < classes
    for q in range(nch):
        here = pl.ds(q * ck, ck)
        z2 = accs[0, pl.ds(0, cpad), here] + precv_thin[0, :, here]
        top = jnp.max(jnp.where(real, z2, -jnp.inf), axis=0, keepdims=True)
        total = jnp.sum(jnp.where(real, jnp.exp(z2 - top), 0.0), axis=0, keepdims=True)
        log_norm = top + jnp.log(total)
        hot = cls == lab_ref[:, here]
        picked = jnp.sum(jnp.where(hot, z2, 0.0), axis=0, keepdims=True)
        mask_f = msk_ref[:, here].astype(F32)
        loss_part += jnp.sum(mask_f * (log_norm - picked), axis=1, keepdims=True)
        soft = jnp.exp(z2 - log_norm)
        g2 = (soft - hot.astype(F32)) * (mask_f / count)
        thin[1, me, q] = jnp.where(real, g2, 0.0).astype(BF)
    run_pass(2, cpad, thin.at[1], precv_thin.at[1])

    d2 = jnp.zeros((cpad, hidden), F32)
    for q in range(nch):
        here = pl.ds(q * ck, ck)
        e2 = (accs[0, pl.ds(0, cpad), here] + precv_thin[1, :, here]).astype(BF)
        d2 += dot_nt(e2, h1[:, here])
        gh = dot_nn(w2b, e2)
        wide[me, q] = jnp.where(h1[:, here] > 0, gh, 0.0).astype(BF)
    row = lax.broadcasted_iota(jnp.int32, (cpad, hidden), 0)
    fin[pl.ds(fin.shape[0] - hidden, hidden)] = jnp.zeros((hidden, hidden), F32)
    fin[pl.ds(w8, cpad)] = jnp.where(row == classes, loss_part / count, d2)
    run_pass(3, hidden, wide, precv)

    for q in range(nch):
        here = pl.ds(q * ck, ck)
        h1[:, here] = (accs[0, :, here] + precv[:, here]).astype(BF)
    fin[pl.ds(0, width)] = dot_nt(xbuf[...], h1[...])

    hh, qq = fin.shape[0] // 2, fin.shape[0] // 8
    c0 = rdma(fin.at[pl.ds(pl.multiple_of(other * hh, hh), hh)], fr1, f_send.at[0], f_recv.at[0], part)
    c0.start()
    c0.wait()
    half[...] = fin[pl.ds(pl.multiple_of(core * hh, hh), hh)] + fr1[...]
    copies = []
    for i, (c, dev) in enumerate(((zc, zs), (xc, xs), (yc, ys))):
        cp = rdma(half.at[pl.ds(pl.multiple_of(c * qq, qq), qq)], fr2.at[i], f_send.at[1 + i], f_recv.at[1 + i], dev)
        cp.start()
        copies.append(cp)
    for cp in copies:
        cp.wait()
    mine = half[pl.ds(pl.multiple_of(chip * qq, qq), qq)] + (fr2[0] + fr2[1] + fr2[2])
    fin_all[me] = mine
    copies = []
    for i, dev in enumerate((zs, xs, ys, part)):
        cp = rdma(fin_all.at[me], fin_all.at[me], f_send.at[4 + i], f_recv.at[4 + i], dev)
        cp.start()
        copies.append(cp)
    back = []
    for i, dev in ((1, xs), (2, ys), (0, zs)):
        rdma(fin_all.at[dev], fin_all.at[dev], f_send.at[4 + i], f_recv.at[4 + i], me).wait_recv()
        cp = rdma(fin_all.at[dev], fin_all.at[dev], f_send.at[8 + i], f_recv.at[8 + i], part)
        cp.start()
        back.append(cp)
    rdma(fin_all.at[part], fin_all.at[part], f_send.at[7], f_recv.at[7], me).wait_recv()
    for i, dev in ((1, xo), (2, yo), (0, zo)):
        rdma(fin_all.at[dev], fin_all.at[dev], f_send.at[8 + i], f_recv.at[8 + i], me).wait_recv()
    for cp in copies + back:
        cp.wait_send()
    for d in range(8):
        out_ref[pl.ds((d % 2) * hh + (d // 2) * qq, qq)] = fin_all[d]


def solution(mesh):
    def local_step(adj_rows, feat_rows, w_one, w_two, label_rows, mask_rows):
        rows, nodes = adj_rows.shape
        width, hidden = w_one.shape
        classes = w_two.shape[1]
        cpad = (classes + 1 + 15) // 16 * 16
        ck = rows // 4
        w8 = (width + 7) // 8 * 8
        fr = (w8 + cpad + 63) // 64 * 64
        dims = (rows, width, hidden, classes)
        vm = pl.BlockSpec(memory_space=pltpu.VMEM)
        hb = pl.BlockSpec(memory_space=pl.ANY)
        dma = pltpu.SemaphoreType.DMA
        with jax.named_scope("gcn"):
            out = pl.pallas_call(
                functools.partial(kernel, dims),
                out_shape=jax.ShapeDtypeStruct((fr, hidden), F32),
                in_specs=[hb, hb, vm, vm, vm, vm],
                out_specs=vm,
                scratch_shapes=[
                    pltpu.VMEM((NB, rows, ck), BF),
                    pltpu.VMEM((20, rows, ck), BF),
                    pltpu.VMEM((8, 4, hidden, ck), BF),
                    pltpu.VMEM((2, 8, 4, cpad, ck), BF),
                    pltpu.VMEM((2, hidden, rows), F32),
                    pltpu.VMEM((hidden, rows), F32),
                    pltpu.VMEM((2, cpad, rows), F32),
                    pltpu.VMEM((width, rows), BF),
                    pltpu.VMEM((hidden, rows), BF),
                    pltpu.VMEM((8, 128), F32),
                    pltpu.VMEM((8, 8, 128), F32),
                    pltpu.VMEM((hidden, 128), F32),
                    pltpu.VMEM((fr, hidden), F32),
                    pltpu.VMEM((fr // 2, hidden), F32),
                    pltpu.VMEM((fr // 2, hidden), F32),
                    pltpu.VMEM((3, fr // 8, hidden), F32),
                    pltpu.VMEM((8, fr // 8, hidden), F32),
                    dma((NB,)), dma((20,)), dma,
                    dma((4, 6, 4)), dma((4, 6, 4)), dma((4,)), dma((4,)), dma((8,)), dma((8,)), dma((11,)), dma((11,)),
                ],
                compiler_params=pltpu.CompilerParams(
                    collective_id=0, has_side_effects=True, vmem_limit_bytes=67043328
                ),
            )(adj_rows, feat_rows.T, w_one, w_two.T, label_rows.reshape(1, rows), mask_rows.reshape(1, rows))
        return out[w8 + classes, 0], out[:width], out[w8:w8 + classes].T

    ax = mesh.axis_names[0]
    return jax.shard_map(local_step, mesh=mesh, in_specs=(P(ax, None), P(ax, None), P(None, None), P(None, None), P(ax), P(ax)),
                         out_specs=(P(), P(None, None), P(None, None)), check_vma=False)
```

```python
import functools

import jax
import jax.numpy as jnp
from jax import lax
from jax.experimental import pallas as pl
from jax.experimental.pallas import tpu as pltpu
from jax.sharding import PartitionSpec as P

BF = jnp.bfloat16
F32 = jnp.float32
MESH = pl.DeviceIdType.MESH
NB = 4
XS, YS, XO, YO, ZS, ZO = range(6)


def dot_nn(a, b):
    return lax.dot_general(a, b, (((1,), (0,)), ((), ())), preferred_element_type=F32)


def dot_nt(a, b):
    return lax.dot_general(a, b, (((1,), (1,)), ((), ())), preferred_element_type=F32)


def kernel(dims, adj, feat, tail_ref, w1_ref, w2_ref, lab_ref, msk_ref, out_ref,
           ring, res, wide, thin, accs, precv, precv_thin, h1, cnt_s, cnt_r, w2p,
           fin, fr1, fr2, fin_all,
           ring_sem, x_sem, g_send, g_recv, p_send, p_recv, c_send, c_recv, f_send, f_recv):
    rows, width, hidden, classes = dims
    cpad = thin.shape[3]
    whole = width // 8 * 8
    w8 = (width + 7) // 8 * 8
    nch = 4
    ck = rows // nch
    me = lax.axis_index("nodes")
    core = lax.rem(me, 2)
    chip = me // 2
    xc = chip + 1 - 2 * lax.rem(chip, 2)
    yc = lax.rem(chip + 2, 4)
    zc = 3 - chip
    other = 1 - core
    part = chip * 2 + other
    xs, xo, ys, yo, zs, zo = (xc * 2 + core, xc * 2 + other, yc * 2 + core, yc * 2 + other,
                              zc * 2 + core, zc * 2 + other)
    dev_of = (xs, ys, xo, yo, zs, zo)

    def item(slot, e, q):
        cols = pl.ds(pl.multiple_of(e * rows + q * ck, ck), ck)
        return pltpu.make_async_copy(adj.at[:, cols], ring.at[slot], ring_sem.at[slot])

    def local_item(m):
        return item(lax.rem(m, NB), me + (m // nch) * (part - me), lax.rem(m, nch))

    near_dev = (xs, ys, xo, yo)

    def x_copies(u):
        more = whole - ck
        return (pltpu.make_async_copy(feat.at[pl.ds(0, ck)], res.at[u], x_sem.at[0]),
                pltpu.make_async_copy(feat.at[pl.ds(ck, more)], res.at[u + 1, pl.ds(0, more)], x_sem.at[1]))

    for cp in x_copies(16):
        cp.start()

    barrier = pltpu.get_barrier_semaphore()
    for o in range(1, 8):
        pl.semaphore_signal(barrier, inc=1, device_id=(lax.rem(me + o, 8),), device_id_type=MESH)

    mask_f = msk_ref[...].astype(F32)
    cnt_s[...] = jnp.broadcast_to(jnp.sum(mask_f, axis=1, keepdims=True), (8, 128))
    w1t = w1_ref[...].astype(BF).T
    w2p[...] = jnp.zeros_like(w2p)
    w2p[pl.ds(0, classes)] = w2_ref[...]
    w2t = w2p[pl.ds(0, cpad)].astype(BF)
    w2b = w2p[...].T[:, :cpad].astype(BF)
    for cp in x_copies(16):
        cp.wait()
    for t in range(NB):
        local_item(t).start()
    pl.semaphore_wait(barrier, 7)

    def cnt_copy(o):
        return pltpu.make_async_remote_copy(cnt_s, cnt_r.at[o], c_send.at[o], c_recv.at[o],
                                            device_id=(lax.rem(me + o, 8),), device_id_type=MESH)

    def rdma(src, dst, ss, rs, dev):
        return pltpu.make_async_remote_copy(src, dst, ss, rs, device_id=(dev,), device_id_type=MESH)

    def gather_send(pi, buf):
        for q in range(nch):
            rdma(buf.at[me, q], buf.at[me, q], g_send.at[pi, 0, q], g_recv.at[pi, XS, q], xs).start()
            rdma(buf.at[me, q], buf.at[me, q], g_send.at[pi, 1, q], g_recv.at[pi, YS, q], ys).start()

    def run_pass(pi, n, buf, prv):
        gather_send(pi, buf)
        if pi > 0:
            accs[:, pl.ds(0, n)] = jnp.zeros((2, n, rows), F32)
        if pi == 0:
            for o in range(1, 8):
                cnt_copy(o).start()

        def local_unit(m):
            b, q = m // nch, lax.rem(m, nch)
            slot = lax.rem(m, NB)
            total = dot_nn(buf[me, 0], ring[slot, pl.ds(0, ck)])
            for c in range(1, nch):
                total += dot_nn(buf[me, c], ring[slot, pl.ds(c * ck, ck)])
            here = pl.ds(pl.multiple_of(q * ck, ck), ck)
            if pi > 0:
                total += accs[b, pl.ds(0, n), here]
            accs[b, pl.ds(0, n), here] = total

        p_copy = rdma(accs.at[1, pl.ds(0, n)], prv, p_send.at[pi], p_recv.at[pi], part)

        def recv(r, q):
            return rdma(buf.at[dev_of[r], q], buf.at[dev_of[r], q], g_send.at[pi, 0, q], g_recv.at[pi, r, q], me)

        def relay(r, q):
            to = {XS: XO, YS: YO, ZS: ZO}[r]
            return rdma(buf.at[dev_of[r], q], buf.at[dev_of[r], q], g_send.at[pi, {XS: 2, YS: 3, ZS: 4}[r], q],
                        g_recv.at[pi, to, q], part)

        def forward(q, src, to):
            return rdma(buf.at[src, q], buf.at[src, q], g_send.at[pi, 5, q], g_recv.at[pi, ZS, q], to)

        def add(*units):
            for i in range(nch):
                here = pl.ds(i * ck, ck)
                s = accs[0, pl.ds(0, n), here]
                for r, q in units:
                    s += dot_nn(buf[dev_of[r], q], res[r * nch + q, :, here])
                accs[0, pl.ds(0, n), here] = s

        def add_new(r, q, slot):
            for i in range(nch):
                here = pl.ds(i * ck, ck)
                t = ring[slot, here, :].T
                res[r * nch + q, :, here] = t
                accs[0, pl.ds(0, n), here] += dot_nn(buf[dev_of[r], q], t)

        def add_far(q, slot):
            for i in range(nch):
                here = pl.ds(i * ck, ck)
                accs[0, pl.ds(0, n), here] += dot_nt(buf[zo, q], ring[slot, here, :])

        def arrivals(q):
            recv(XS, q).wait_recv()
            relay(XS, q).start()

            @pl.when(q < 2)
            def _():
                forward(q, xs, ys).start()
            recv(YS, q).wait_recv()
            relay(YS, q).start()

            @pl.when(q >= 2)
            def _():
                forward(q, ys, xs).start()

        def far_arrival(q):
            recv(ZS, q).wait_recv()
            relay(ZS, q).start()

        if pi == 0:
            def local(m, _):
                local_item(m).wait()
                local_unit(m)

                @pl.when(m < 4)
                def _():
                    local_item(m + 4).start()
                for j in range(4):
                    @pl.when(m == 4 + j)
                    def _(j=j):
                        item(j, near_dev[j], 0).start()
                return 0

            lax.fori_loop(0, 8, local, 0)
            p_copy.start()

            def near(q, _):
                arrivals(q)

                @pl.when(q >= 2)
                def _():
                    far_arrival(q - 2)
                for j, r in enumerate((XS, YS, XO, YO)):
                    if j >= 2:
                        recv(r, q).wait_recv()
                    item(j, near_dev[j], q).wait()
                    add_new(r, q, j)

                    @pl.when(q < 3)
                    def _(j=j):
                        item(j, near_dev[j], q + 1).start()

                    @pl.when(q == 3)
                    def _(j=j):
                        item(j, (zs, zo)[j % 2], j // 2).start()
                return 0

            lax.fori_loop(0, nch, near, 0)

            def far(q, _):
                @pl.when(q < 2)
                def _():
                    far_arrival(q + 2)
                for j in range(2):
                    slot = lax.rem(2 * q + j, NB)
                    item(slot, (zs, zo)[j], q).wait()
                    if j == 0:
                        add_new(ZS, q, slot)
                    else:
                        recv(ZO, q).wait_recv()
                        add_far(q, slot)

                    @pl.when(q < 2)
                    def _(j=j, slot=slot):
                        item(slot, (zs, zo)[j], q + 2).start()

                    @pl.when(q >= 2)
                    def _(j=j):
                        local_item(2 * (q - 2) + j).start()
                return 0

            lax.fori_loop(0, nch, far, 0)
        else:
            def near(q, _):
                arrivals(q)

                @pl.when(q >= 2)
                def _():
                    far_arrival(q - 2)
                local_item(2 * q).wait()
                local_item(2 * q + 1).wait()
                local_unit(2 * q)
                local_unit(2 * q + 1)

                @pl.when(q < 2)
                def _():
                    local_item(2 * q + 4).start()
                    local_item(2 * q + 5).start()

                @pl.when(q >= 2)
                def _():
                    item(2 * q - 4, zo, 2 * q - 4).start()
                    item(2 * q - 3, zo, 2 * q - 3).start()

                @pl.when(q == 3)
                def _():
                    p_copy.start()
                add((XS, q), (YS, q))
                recv(XO, q).wait_recv()
                recv(YO, q).wait_recv()
                add((XO, q), (YO, q))
                return 0

            lax.fori_loop(0, nch, near, 0)
            if pi == 3:
                for cp in x_copies(0):
                    cp.start()

            def far(q, _):
                @pl.when(q < 2)
                def _():
                    far_arrival(q + 2)
                item(q, zo, q).wait()
                recv(ZO, q).wait_recv()
                add((ZS, q))
                add_far(q, q)
                if pi < 3:
                    local_item(q).start()
                return 0

            lax.fori_loop(0, nch, far, 0)

        def drain(q, _):
            for i in range(6):
                rdma(buf.at[me, q], buf.at[me, q], g_send.at[pi, i, q], g_recv.at[pi, 0, q], me).wait_send()
            return 0

        lax.fori_loop(0, nch, drain, 0)
        p_copy.wait()

    for q in range(nch):
        here = pl.ds(q * ck, ck)
        y1 = dot_nn(w1t[:, :ck], res[16, :, here])
        y1 += dot_nn(w1t[:, ck:whole], res[17, pl.ds(0, whole - ck), here])
        y1 += dot_nn(w1t[:, whole:], tail_ref[pl.ds(0, width - whole), here])
        wide[me, q] = y1.astype(BF)
    run_pass(0, hidden, wide, precv)

    for q in range(nch):
        here = pl.ds(q * ck, ck)
        h = jnp.maximum(accs[0, :, here] + precv[:, here], 0.0).astype(BF)
        h1[:, here] = h
        thin[0, me, q] = dot_nn(w2t, h).astype(BF)
    run_pass(1, cpad, thin.at[0], precv_thin.at[0])

    count = cnt_s[...]
    for o in range(1, 8):
        cnt_copy(o).wait()
        count += cnt_r[o]
    count = count[0:1, 0:1]
    loss_part = jnp.zeros((1, 1), F32)
    cls = lax.broadcasted_iota(jnp.int32, (cpad, ck), 0)
    real = cls < classes
    for q in range(nch):
        here = pl.ds(q * ck, ck)
        z2 = accs[0, pl.ds(0, cpad), here] + precv_thin[0, :, here]
        top = jnp.max(jnp.where(real, z2, -jnp.inf), axis=0, keepdims=True)
        total = jnp.sum(jnp.where(real, jnp.exp(z2 - top), 0.0), axis=0, keepdims=True)
        log_norm = top + jnp.log(total)
        hot = cls == lab_ref[:, here]
        picked = jnp.sum(jnp.where(hot, z2, 0.0), axis=0, keepdims=True)
        mask_f = msk_ref[:, here].astype(F32)
        loss_part += jnp.sum(mask_f * (log_norm - picked), axis=1, keepdims=True)
        soft = jnp.exp(z2 - log_norm)
        g2 = (soft - hot.astype(F32)) * (mask_f / count)
        thin[1, me, q] = jnp.where(real, g2, 0.0).astype(BF)
    run_pass(2, cpad, thin.at[1], precv_thin.at[1])

    d2 = jnp.zeros((cpad, hidden), F32)
    for q in range(nch):
        here = pl.ds(q * ck, ck)
        e2 = (accs[0, pl.ds(0, cpad), here] + precv_thin[1, :, here]).astype(BF)
        d2 += dot_nt(e2, h1[:, here])
        gh = dot_nn(w2b, e2)
        wide[me, q] = jnp.where(h1[:, here] > 0, gh, 0.0).astype(BF)
    row = lax.broadcasted_iota(jnp.int32, (cpad, hidden), 0)
    fin[pl.ds(fin.shape[0] - hidden, hidden)] = jnp.zeros((hidden, hidden), F32)
    fin[pl.ds(w8, cpad)] = jnp.where(row == classes, loss_part / count, d2)
    run_pass(3, hidden, wide, precv)

    for q in range(nch):
        here = pl.ds(q * ck, ck)
        h1[:, here] = (accs[0, :, here] + precv[:, here]).astype(BF)
    for cp in x_copies(0):
        cp.wait()
    fin[pl.ds(0, ck)] = dot_nt(res[0], h1[...])
    fin[pl.ds(ck, whole - ck)] = dot_nt(res[1, pl.ds(0, whole - ck)], h1[...])
    fin[pl.ds(whole, 8)] = dot_nt(tail_ref[...], h1[...])

    hh, qq = fin.shape[0] // 2, fin.shape[0] // 8
    c0 = rdma(fin.at[pl.ds(pl.multiple_of(other * hh, hh), hh)], fr1, f_send.at[0], f_recv.at[0], part)
    c0.start()
    c0.wait()
    half = fr1
    half[...] += fin[pl.ds(pl.multiple_of(core * hh, hh), hh)]
    copies = []
    for i, (c, dev) in enumerate(((zc, zs), (xc, xs), (yc, ys))):
        cp = rdma(half.at[pl.ds(pl.multiple_of(c * qq, qq), qq)], fr2.at[i], f_send.at[1 + i], f_recv.at[1 + i], dev)
        cp.start()
        copies.append(cp)
    for cp in copies:
        cp.wait()
    mine = half[pl.ds(pl.multiple_of(chip * qq, qq), qq)] + (fr2[0] + fr2[1] + fr2[2])
    fin_all[me] = mine
    copies = []
    for i, dev in enumerate((zs, xs, ys, part)):
        cp = rdma(fin_all.at[me], fin_all.at[me], f_send.at[4 + i], f_recv.at[4 + i], dev)
        cp.start()
        copies.append(cp)
    back = []
    for i, dev in ((1, xs), (2, ys), (0, zs)):
        rdma(fin_all.at[dev], fin_all.at[dev], f_send.at[4 + i], f_recv.at[4 + i], me).wait_recv()
        cp = rdma(fin_all.at[dev], fin_all.at[dev], f_send.at[8 + i], f_recv.at[8 + i], part)
        cp.start()
        back.append(cp)
    rdma(fin_all.at[part], fin_all.at[part], f_send.at[7], f_recv.at[7], me).wait_recv()
    for i, dev in ((1, xo), (2, yo), (0, zo)):
        rdma(fin_all.at[dev], fin_all.at[dev], f_send.at[8 + i], f_recv.at[8 + i], me).wait_recv()
    for cp in copies + back:
        cp.wait_send()
    for d in range(8):
        out_ref[pl.ds((d % 2) * hh + (d // 2) * qq, qq)] = fin_all[d]


def solution(mesh):
    def local_step(adj_rows, feat_rows, w_one, w_two, label_rows, mask_rows):
        rows, nodes = adj_rows.shape
        width, hidden = w_one.shape
        classes = w_two.shape[1]
        cpad = (classes + 1 + 15) // 16 * 16
        ck = rows // 4
        w8 = (width + 7) // 8 * 8
        fr = (w8 + cpad + 63) // 64 * 64
        dims = (rows, width, hidden, classes)
        vm = pl.BlockSpec(memory_space=pltpu.VMEM)
        hb = pl.BlockSpec(memory_space=pl.ANY)
        dma = pltpu.SemaphoreType.DMA
        tail = feat_rows.T[width // 8 * 8:]
        tail = jnp.pad(tail, ((0, 8 - tail.shape[0]), (0, 0)))
        with jax.named_scope("gcn"):
            out = pl.pallas_call(
                functools.partial(kernel, dims),
                out_shape=jax.ShapeDtypeStruct((fr, hidden), F32),
                in_specs=[hb, hb, vm, vm, vm, vm, vm],
                out_specs=vm,
                scratch_shapes=[
                    pltpu.VMEM((NB, rows, ck), BF),
                    pltpu.VMEM((20, ck, rows), BF),
                    pltpu.VMEM((8, 4, hidden, ck), BF),
                    pltpu.VMEM((2, 8, 4, cpad, ck), BF),
                    pltpu.VMEM((2, hidden, rows), F32),
                    pltpu.VMEM((hidden, rows), F32),
                    pltpu.VMEM((2, cpad, rows), F32),
                    pltpu.VMEM((hidden, rows), BF),
                    pltpu.VMEM((8, 128), F32),
                    pltpu.VMEM((8, 8, 128), F32),
                    pltpu.VMEM((hidden, 128), F32),
                    pltpu.VMEM((fr, hidden), F32),
                    pltpu.VMEM((fr // 2, hidden), F32),
                    pltpu.VMEM((3, fr // 8, hidden), F32),
                    pltpu.VMEM((8, fr // 8, hidden), F32),
                    dma((NB,)), dma((2,)),
                    dma((4, 6, 4)), dma((4, 6, 4)), dma((4,)), dma((4,)), dma((8,)), dma((8,)), dma((11,)), dma((11,)),
                ],
                compiler_params=pltpu.CompilerParams(
                    collective_id=0, has_side_effects=True, vmem_limit_bytes=67043328
                ),
            )(adj_rows, feat_rows.T, tail, w_one, w_two.T, label_rows.reshape(1, rows), mask_rows.reshape(1, rows))
        return out[w8 + classes, 0], out[:width], out[w8:w8 + classes].T

    ax = mesh.axis_names[0]
    return jax.shard_map(local_step, mesh=mesh, in_specs=(P(ax, None), P(ax, None), P(None, None), P(None, None), P(ax), P(ax)),
                         out_specs=(P(), P(None, None), P(None, None)), check_vma=False)
```

```python
import functools

import jax
import jax.numpy as jnp
from jax import lax
from jax.experimental import pallas as pl
from jax.experimental.pallas import tpu as pltpu
from jax.sharding import PartitionSpec as P

BF = jnp.bfloat16
F32 = jnp.float32
MESH = pl.DeviceIdType.MESH
NB = 4
XS, YS, XO, YO, ZS, ZO = range(6)


def dot_nn(a, b):
    return lax.dot_general(a, b, (((1,), (0,)), ((), ())), preferred_element_type=F32)


def dot_nt(a, b):
    return lax.dot_general(a, b, (((1,), (1,)), ((), ())), preferred_element_type=F32)


def kernel(dims, adj, feat, tail_ref, w1_ref, w2_ref, lab_ref, msk_ref, out_ref,
           ring, res, wide, thin, accs, precv, precv_thin, h1, cnt_s, cnt_r, w2p,
           fin, fr1, fr2, fin_all,
           ring_sem, x_sem, g_send, g_recv, p_send, p_recv, c_send, c_recv, f_send, f_recv):
    rows, width, hidden, classes = dims
    cpad = thin.shape[3]
    whole = width // 8 * 8
    w8 = (width + 7) // 8 * 8
    nch = 4
    ck = rows // nch
    me = lax.axis_index("nodes")
    core = lax.rem(me, 2)
    chip = me // 2
    xc = chip + 1 - 2 * lax.rem(chip, 2)
    yc = lax.rem(chip + 2, 4)
    zc = 3 - chip
    other = 1 - core
    part = chip * 2 + other
    xs, xo, ys, yo, zs, zo = (xc * 2 + core, xc * 2 + other, yc * 2 + core, yc * 2 + other,
                              zc * 2 + core, zc * 2 + other)
    dev_of = (xs, ys, xo, yo, zs, zo)

    def item(slot, e, q):
        cols = pl.ds(pl.multiple_of(e * rows + q * ck, ck), ck)
        return pltpu.make_async_copy(adj.at[:, cols], ring.at[slot], ring_sem.at[slot])

    def local_item(m):
        return item(lax.rem(m, NB), me + (m // nch) * (part - me), lax.rem(m, nch))

    near_dev = (xs, ys, xo, yo)

    def x_copies(u):
        more = whole - ck
        return (pltpu.make_async_copy(feat.at[pl.ds(0, ck)], res.at[u], x_sem.at[0]),
                pltpu.make_async_copy(feat.at[pl.ds(ck, more)], res.at[u + 1, pl.ds(0, more)], x_sem.at[1]))

    for cp in x_copies(16):
        cp.start()

    barrier = pltpu.get_barrier_semaphore()
    for o in range(1, 8):
        pl.semaphore_signal(barrier, inc=1, device_id=(lax.rem(me + o, 8),), device_id_type=MESH)

    mask_f = msk_ref[...].astype(F32)
    cnt_s[...] = jnp.broadcast_to(jnp.sum(mask_f, axis=1, keepdims=True), (8, 128))
    w1t = w1_ref[...].astype(BF).T
    w2p[...] = jnp.zeros_like(w2p)
    w2p[pl.ds(0, classes)] = w2_ref[...]
    w2t = w2p[pl.ds(0, cpad)].astype(BF)
    w2b = w2p[...].T[:, :cpad].astype(BF)
    for cp in x_copies(16):
        cp.wait()
    for t in range(NB):
        local_item(t).start()
    with jax.named_scope("barrier"):
        pl.semaphore_wait(barrier, 7)

    def cnt_copy(o):
        return pltpu.make_async_remote_copy(cnt_s, cnt_r.at[o], c_send.at[o], c_recv.at[o],
                                            device_id=(lax.rem(me + o, 8),), device_id_type=MESH)

    def rdma(src, dst, ss, rs, dev):
        return pltpu.make_async_remote_copy(src, dst, ss, rs, device_id=(dev,), device_id_type=MESH)

    def gather_send(pi, buf):
        for q in range(nch):
            rdma(buf.at[me, q], buf.at[me, q], g_send.at[pi, 0, q], g_recv.at[pi, XS, q], xs).start()
            rdma(buf.at[me, q], buf.at[me, q], g_send.at[pi, 1, q], g_recv.at[pi, YS, q], ys).start()

    def run_pass(pi, n, buf, prv):
        gather_send(pi, buf)
        if pi > 0:
            accs[:, pl.ds(0, n)] = jnp.zeros((2, n, rows), F32)
        if pi == 0:
            for o in range(1, 8):
                cnt_copy(o).start()

        def local_unit(m):
            b, q = m // nch, lax.rem(m, nch)
            slot = lax.rem(m, NB)
            total = dot_nn(buf[me, 0], ring[slot, pl.ds(0, ck)])
            for c in range(1, nch):
                total += dot_nn(buf[me, c], ring[slot, pl.ds(c * ck, ck)])
            here = pl.ds(pl.multiple_of(q * ck, ck), ck)
            if pi > 0:
                total += accs[b, pl.ds(0, n), here]
            accs[b, pl.ds(0, n), here] = total

        p_copy = rdma(accs.at[1, pl.ds(0, n)], prv, p_send.at[pi], p_recv.at[pi], part)

        def recv(r, q):
            return rdma(buf.at[dev_of[r], q], buf.at[dev_of[r], q], g_send.at[pi, 0, q], g_recv.at[pi, r, q], me)

        def relay(r, q):
            to = {XS: XO, YS: YO, ZS: ZO}[r]
            return rdma(buf.at[dev_of[r], q], buf.at[dev_of[r], q], g_send.at[pi, {XS: 2, YS: 3, ZS: 4}[r], q],
                        g_recv.at[pi, to, q], part)

        def forward(q, src, to):
            return rdma(buf.at[src, q], buf.at[src, q], g_send.at[pi, 5, q], g_recv.at[pi, ZS, q], to)

        def add(*units):
            for i in range(nch):
                here = pl.ds(i * ck, ck)
                s = accs[0, pl.ds(0, n), here]
                for r, q in units:
                    s += dot_nn(buf[dev_of[r], q], res[r * nch + q, :, here])
                accs[0, pl.ds(0, n), here] = s

        def add_new(r, q, slot):
            for i in range(nch):
                here = pl.ds(i * ck, ck)
                t = ring[slot, here, :].T
                res[r * nch + q, :, here] = t
                accs[0, pl.ds(0, n), here] += dot_nn(buf[dev_of[r], q], t)

        def add_far(q, slot):
            for i in range(nch):
                here = pl.ds(i * ck, ck)
                accs[0, pl.ds(0, n), here] += dot_nt(buf[zo, q], ring[slot, here, :])

        def arrivals(q):
            recv(XS, q).wait_recv()
            relay(XS, q).start()

            @pl.when(q < 2)
            def _():
                forward(q, xs, ys).start()
            recv(YS, q).wait_recv()
            relay(YS, q).start()

            @pl.when(q >= 2)
            def _():
                forward(q, ys, xs).start()

        def far_arrival(q):
            recv(ZS, q).wait_recv()
            relay(ZS, q).start()

        if pi == 0:
            def local(m, _):
                local_item(m).wait()
                local_unit(m)

                @pl.when(m < 4)
                def _():
                    local_item(m + 4).start()
                for j in range(4):
                    @pl.when(m == 4 + j)
                    def _(j=j):
                        item(j, near_dev[j], 0).start()
                return 0

            with jax.named_scope(f"local_{pi}"):
                lax.fori_loop(0, 8, local, 0)
            p_copy.start()

            def near(q, _):
                arrivals(q)

                @pl.when(q >= 2)
                def _():
                    far_arrival(q - 2)
                for j, r in enumerate((XS, YS, XO, YO)):
                    if j >= 2:
                        recv(r, q).wait_recv()
                    item(j, near_dev[j], q).wait()
                    add_new(r, q, j)

                    @pl.when(q < 3)
                    def _(j=j):
                        item(j, near_dev[j], q + 1).start()

                    @pl.when(q == 3)
                    def _(j=j):
                        item(j, (zs, zo)[j % 2], j // 2).start()
                return 0

            with jax.named_scope(f"near_{pi}"):
                lax.fori_loop(0, nch, near, 0)

            def far(q, _):
                @pl.when(q < 2)
                def _():
                    far_arrival(q + 2)
                for j in range(2):
                    slot = lax.rem(2 * q + j, NB)
                    item(slot, (zs, zo)[j], q).wait()
                    if j == 0:
                        add_new(ZS, q, slot)
                    else:
                        recv(ZO, q).wait_recv()
                        add_far(q, slot)

                    @pl.when(q < 2)
                    def _(j=j, slot=slot):
                        item(slot, (zs, zo)[j], q + 2).start()

                    @pl.when(q >= 2)
                    def _(j=j):
                        local_item(2 * (q - 2) + j).start()
                return 0

            with jax.named_scope(f"far_{pi}"):
                lax.fori_loop(0, nch, far, 0)
        else:
            def local_pair(q):
                local_item(2 * q).wait()
                local_item(2 * q + 1).wait()
                local_unit(2 * q)
                local_unit(2 * q + 1)

            arrivals(0)
            local_pair(0)
            add((XS, 0), (YS, 0))
            local_item(4).start()
            local_item(5).start()

            def near(q, _):
                arrivals(q)
                recv(XO, q - 1).wait_recv()
                recv(YO, q - 1).wait_recv()

                @pl.when(q >= 2)
                def _():
                    far_arrival(q - 2)
                local_pair(q)
                add((XS, q), (YS, q), (XO, q - 1), (YO, q - 1))

                @pl.when(q < 2)
                def _():
                    local_item(2 * q + 4).start()
                    local_item(2 * q + 5).start()

                @pl.when(q >= 2)
                def _():
                    item(2 * q - 4, zo, 2 * q - 4).start()
                    item(2 * q - 3, zo, 2 * q - 3).start()
                return 0

            with jax.named_scope(f"near_{pi}"):
                lax.fori_loop(1, nch, near, 0)
            p_copy.start()
            if pi == 3:
                for cp in x_copies(0):
                    cp.start()
            recv(XO, 3).wait_recv()
            recv(YO, 3).wait_recv()
            far_arrival(2)
            add((XO, 3), (YO, 3), (ZS, 0), (ZS, 1))
            far_arrival(3)

            def far(h, _):
                for q in (2 * h, 2 * h + 1):
                    item(q, zo, q).wait()
                    recv(ZO, q).wait_recv()
                for i in range(nch):
                    here = pl.ds(i * ck, ck)
                    s = accs[0, pl.ds(0, n), here]
                    s += dot_nn(buf[zs, h + 2], res[ZS * nch + h + 2, :, here])
                    for q in (2 * h, 2 * h + 1):
                        s += dot_nt(buf[zo, q], ring[q, here, :])
                    accs[0, pl.ds(0, n), here] = s
                if pi < 3:
                    for q in (2 * h, 2 * h + 1):
                        local_item(q).start()
                return 0

            with jax.named_scope(f"far_{pi}"):
                lax.fori_loop(0, 2, far, 0)

        def drain(q, _):
            for i in range(6):
                rdma(buf.at[me, q], buf.at[me, q], g_send.at[pi, i, q], g_recv.at[pi, 0, q], me).wait_send()
            return 0

        lax.fori_loop(0, nch, drain, 0)
        p_copy.wait()

    for q in range(nch):
        here = pl.ds(q * ck, ck)
        y1 = dot_nn(w1t[:, :ck], res[16, :, here])
        y1 += dot_nn(w1t[:, ck:whole], res[17, pl.ds(0, whole - ck), here])
        y1 += dot_nn(w1t[:, whole:], tail_ref[pl.ds(0, width - whole), here])
        wide[me, q] = y1.astype(BF)
    with jax.named_scope("pass_0"):
        run_pass(0, hidden, wide, precv)

    for q in range(nch):
        here = pl.ds(q * ck, ck)
        h = jnp.maximum(accs[0, :, here] + precv[:, here], 0.0).astype(BF)
        h1[:, here] = h
        thin[0, me, q] = dot_nn(w2t, h).astype(BF)
    with jax.named_scope("pass_1"):
        run_pass(1, cpad, thin.at[0], precv_thin.at[0])

    count = cnt_s[...]
    for o in range(1, 8):
        cnt_copy(o).wait()
        count += cnt_r[o]
    count = count[0:1, 0:1]
    loss_part = jnp.zeros((1, 1), F32)
    cls = lax.broadcasted_iota(jnp.int32, (cpad, ck), 0)
    real = cls < classes
    for q in range(nch):
        here = pl.ds(q * ck, ck)
        z2 = accs[0, pl.ds(0, cpad), here] + precv_thin[0, :, here]
        top = jnp.max(jnp.where(real, z2, -jnp.inf), axis=0, keepdims=True)
        total = jnp.sum(jnp.where(real, jnp.exp(z2 - top), 0.0), axis=0, keepdims=True)
        log_norm = top + jnp.log(total)
        hot = cls == lab_ref[:, here]
        picked = jnp.sum(jnp.where(hot, z2, 0.0), axis=0, keepdims=True)
        mask_f = msk_ref[:, here].astype(F32)
        loss_part += jnp.sum(mask_f * (log_norm - picked), axis=1, keepdims=True)
        soft = jnp.exp(z2 - log_norm)
        g2 = (soft - hot.astype(F32)) * (mask_f / count)
        thin[1, me, q] = jnp.where(real, g2, 0.0).astype(BF)
    with jax.named_scope("pass_2"):
        run_pass(2, cpad, thin.at[1], precv_thin.at[1])

    d2 = jnp.zeros((cpad, hidden), F32)
    for q in range(nch):
        here = pl.ds(q * ck, ck)
        e2 = (accs[0, pl.ds(0, cpad), here] + precv_thin[1, :, here]).astype(BF)
        d2 += dot_nt(e2, h1[:, here])
        gh = dot_nn(w2b, e2)
        wide[me, q] = jnp.where(h1[:, here] > 0, gh, 0.0).astype(BF)
    row = lax.broadcasted_iota(jnp.int32, (cpad, hidden), 0)
    fin[pl.ds(fin.shape[0] - hidden, hidden)] = jnp.zeros((hidden, hidden), F32)
    fin[pl.ds(w8, cpad)] = jnp.where(row == classes, loss_part / count, d2)
    with jax.named_scope("pass_3"):
        run_pass(3, hidden, wide, precv)

    for q in range(nch):
        here = pl.ds(q * ck, ck)
        h1[:, here] = (accs[0, :, here] + precv[:, here]).astype(BF)
    for cp in x_copies(0):
        cp.wait()
    fin[pl.ds(0, ck)] = dot_nt(res[0], h1[...])
    fin[pl.ds(ck, whole - ck)] = dot_nt(res[1, pl.ds(0, whole - ck)], h1[...])
    fin[pl.ds(whole, 8)] = dot_nt(tail_ref[...], h1[...])

    hh, qq = fin.shape[0] // 2, fin.shape[0] // 8
    c0 = rdma(fin.at[pl.ds(pl.multiple_of(other * hh, hh), hh)], fr1, f_send.at[0], f_recv.at[0], part)
    c0.start()
    with jax.named_scope("c0"):
        c0.wait()
    half = fr1
    half[...] += fin[pl.ds(pl.multiple_of(core * hh, hh), hh)]
    copies = []
    for i, (c, dev) in enumerate(((zc, zs), (xc, xs), (yc, ys))):
        cp = rdma(half.at[pl.ds(pl.multiple_of(c * qq, qq), qq)], fr2.at[i], f_send.at[1 + i], f_recv.at[1 + i], dev)
        cp.start()
        copies.append(cp)
    with jax.named_scope("c1"):
        for cp in copies:
            cp.wait()
    mine = half[pl.ds(pl.multiple_of(chip * qq, qq), qq)] + (fr2[0] + fr2[1] + fr2[2])
    fin_all[me] = mine
    copies = []
    for i, dev in enumerate((zs, xs, ys, part)):
        cp = rdma(fin_all.at[me], fin_all.at[me], f_send.at[4 + i], f_recv.at[4 + i], dev)
        cp.start()
        copies.append(cp)
    back = []
    for i, dev in ((1, xs), (2, ys), (0, zs)):
        rdma(fin_all.at[dev], fin_all.at[dev], f_send.at[4 + i], f_recv.at[4 + i], me).wait_recv()
        cp = rdma(fin_all.at[dev], fin_all.at[dev], f_send.at[8 + i], f_recv.at[8 + i], part)
        cp.start()
        back.append(cp)
    with jax.named_scope("c2"):
        rdma(fin_all.at[part], fin_all.at[part], f_send.at[7], f_recv.at[7], me).wait_recv()
    for i, dev in ((1, xo), (2, yo), (0, zo)):
        rdma(fin_all.at[dev], fin_all.at[dev], f_send.at[8 + i], f_recv.at[8 + i], me).wait_recv()
    for cp in copies + back:
        cp.wait_send()
    for d in range(8):
        out_ref[pl.ds((d % 2) * hh + (d // 2) * qq, qq)] = fin_all[d]


def solution(mesh):
    def local_step(adj_rows, feat_rows, w_one, w_two, label_rows, mask_rows):
        rows, nodes = adj_rows.shape
        width, hidden = w_one.shape
        classes = w_two.shape[1]
        cpad = (classes + 1 + 15) // 16 * 16
        ck = rows // 4
        w8 = (width + 7) // 8 * 8
        fr = (w8 + cpad + 63) // 64 * 64
        dims = (rows, width, hidden, classes)
        vm = pl.BlockSpec(memory_space=pltpu.VMEM)
        hb = pl.BlockSpec(memory_space=pl.ANY)
        dma = pltpu.SemaphoreType.DMA
        tail = feat_rows.T[width // 8 * 8:]
        tail = jnp.pad(tail, ((0, 8 - tail.shape[0]), (0, 0)))
        with jax.named_scope("gcn"):
            out = pl.pallas_call(
                functools.partial(kernel, dims),
                out_shape=jax.ShapeDtypeStruct((fr, hidden), F32),
                in_specs=[hb, hb, vm, vm, vm, vm, vm],
                out_specs=vm,
                scratch_shapes=[
                    pltpu.VMEM((NB, rows, ck), BF),
                    pltpu.VMEM((20, ck, rows), BF),
                    pltpu.VMEM((8, 4, hidden, ck), BF),
                    pltpu.VMEM((2, 8, 4, cpad, ck), BF),
                    pltpu.VMEM((2, hidden, rows), F32),
                    pltpu.VMEM((hidden, rows), F32),
                    pltpu.VMEM((2, cpad, rows), F32),
                    pltpu.VMEM((hidden, rows), BF),
                    pltpu.VMEM((8, 128), F32),
                    pltpu.VMEM((8, 8, 128), F32),
                    pltpu.VMEM((hidden, 128), F32),
                    pltpu.VMEM((fr, hidden), F32),
                    pltpu.VMEM((fr // 2, hidden), F32),
                    pltpu.VMEM((3, fr // 8, hidden), F32),
                    pltpu.VMEM((8, fr // 8, hidden), F32),
                    dma((NB,)), dma((2,)),
                    dma((4, 6, 4)), dma((4, 6, 4)), dma((4,)), dma((4,)), dma((8,)), dma((8,)), dma((11,)), dma((11,)),
                ],
                compiler_params=pltpu.CompilerParams(
                    collective_id=0, has_side_effects=True, vmem_limit_bytes=67043328
                ),
            )(adj_rows, feat_rows.T, tail, w_one, w_two.T, label_rows.reshape(1, rows), mask_rows.reshape(1, rows))
        return out[w8 + classes, 0], out[:width], out[w8:w8 + classes].T

    ax = mesh.axis_names[0]
    return jax.shard_map(local_step, mesh=mesh, in_specs=(P(ax, None), P(ax, None), P(None, None), P(None, None), P(ax), P(ax)),
                         out_specs=(P(), P(None, None), P(None, None)), check_vma=False)
```
